8 devices in a mesh: dp: 2 (over z, y), tp: 4 (over x, core).
Axes of the slice: x: 2, y: 2, z: 1, core: 2. Of those that a mesh axis runs over, the one named last changes fastest.
Arguments:
- hidden: bfloat16 [12, 8, 4096], P('dp'), parts along dimension 0
- draft_ids: int32 [12, 7], P('dp'), parts along dimension 0
- temperature: float32 [12], P('dp'), parts along dimension 0
- norm_gain: bfloat16 [4096], replicated
- head_weight: bfloat16 [128256, 4096], P('tp')
Outputs:
- output 1: float32 [12, 7], P('dp'), parts along dimension 0
- output 2: float32 [12, 8], P('dp'), parts along dimension 0
- output 3: float32 [12, 8], P('dp'), parts along dimension 0
There are 2 independent parts. The reference program is written for one: setup_inputs(seed, part) draws one part's arguments, and reference() takes and returns one part's arrays. A program takes and returns all parts, laid end to end along the dimension named above; an argument that names none is the same for every part.
All inputs are finite; a program needn't handle non-finite values.
Results may differ from the reference program's by a relative error of at most 0.001.
Values sent between devices are 32-bit elements.
A program may use at most 1 GiB of HBM per device.

```python
import jax
import jax.numpy as jnp
from jax import lax

BATCH_ROWS = 6
DRAFT_LEN = 7
MODEL_DIM = 4096
VOCAB_SIZE = 128256
NORM_EPS = 1e-5


def setup_inputs(seed: int = 0, part: int = 0) -> dict:
    base_key = jax.random.key(seed)
    part_key = jax.random.fold_in(base_key, part)
    key_hidden, key_draft, key_temp = jax.random.split(part_key, 3)
    key_gain, key_head = jax.random.split(jax.random.key(seed + 1), 2)
    hidden = jax.random.normal(key_hidden, (BATCH_ROWS, DRAFT_LEN + 1, MODEL_DIM), jnp.float32).astype(jnp.bfloat16)
    draft_ids = jax.random.randint(key_draft, (BATCH_ROWS, DRAFT_LEN), 0, VOCAB_SIZE, jnp.int32)
    draft_ids = draft_ids.at[0, 0].set(0).at[0, 1].set(VOCAB_SIZE - 1)
    temperature = jax.random.uniform(key_temp, (BATCH_ROWS,), jnp.float32, 0.6, 1.2)
    norm_gain = (1.5 + 0.3 * jax.random.normal(key_gain, (MODEL_DIM,), jnp.float32)).astype(jnp.bfloat16)
    head_weight = (2.0 * MODEL_DIM ** -0.5 * jax.random.normal(key_head, (VOCAB_SIZE, MODEL_DIM), jnp.float32)).astype(jnp.bfloat16)
    return {"hidden": hidden, "draft_ids": draft_ids, "temperature": temperature, "norm_gain": norm_gain, "head_weight": head_weight}


def reference(hidden, draft_ids, temperature, norm_gain, head_weight):
    hidden_f32 = hidden.astype(jnp.float32)
    mean_sq = jnp.mean(hidden_f32 * hidden_f32, axis=-1, keepdims=True)
    normed = (hidden_f32 * lax.rsqrt(mean_sq + NORM_EPS) * norm_gain.astype(jnp.float32)).astype(jnp.bfloat16)

    def per_row(row_args):
        normed_row, draft_row, temp_row = row_args
        logits = jnp.dot(normed_row, head_weight.T, preferred_element_type=jnp.float32) / temp_row
        row_max = jnp.max(logits, axis=-1, keepdims=True)
        shifted = jnp.exp(logits - row_max)
        total = jnp.sum(shifted, axis=-1)
        weighted = jnp.sum(shifted * logits, axis=-1)
        log_norm = row_max[:, 0] + jnp.log(total)
        entropy = log_norm - weighted / total
        picked = jnp.take_along_axis(logits[:DRAFT_LEN], draft_row[:, None], axis=1)[:, 0]
        return picked - log_norm[:DRAFT_LEN], log_norm, entropy

    log_probs, log_norm, entropy = lax.map(per_row, (normed, draft_ids, temperature))
    return log_probs, log_norm, entropy
```

```python
import functools

import jax
import jax.numpy as jnp
from jax import lax
from jax.experimental import pallas as pl
from jax.experimental.pallas import tpu as pltpu
from jax.sharding import PartitionSpec as P

NORM_EPS = 1e-5
LOG2E = 1.4426950408889634
LOWEST = -3.0e38
MESH = pl.DeviceIdType.MESH
TILE = 1024
SLOTS = 6
PRIVATE_TILES = 3
CHUNK = 8


def kernel(
    h_ref, draft_ref, temp_ref, gain_ref, w_ref, lp_ref, lse_ref, ent_ref,
    wbuf, hbuf, gbuf, hsend, hrecv, g, aux, auxin, stats, statsin, draft_s, temp_s,
    wsem, insem, send_sem, recv_sem, fsend_sem, frecv_sem, asem, ssend_sem, srecv_sem,
):
    dp, tp = lax.axis_index("dp"), lax.axis_index("tp")
    core = lax.rem(tp, 2)
    mate = tp + 1 - 2 * core
    rows, dim = w_ref.shape
    tokens = hbuf.shape[0]
    batch, positions = temp_s.shape[1], tokens // temp_s.shape[1]
    shared = (rows - PRIVATE_TILES * TILE) // 2 // TILE * TILE
    private = rows - 2 * shared
    first = private - PRIVATE_TILES * TILE
    total = 1 + PRIVATE_TILES + shared // TILE

    def offset(i):
        return first + (i - 1) * TILE

    def tile_copy(i):
        start = offset(i) + jnp.where(i > PRIVATE_TILES, dp * shared, 0)
        slot = lax.rem(i, SLOTS)
        return pltpu.make_async_copy(
            w_ref.at[pl.ds(pl.multiple_of(start, 64), TILE), :], wbuf.at[slot], wsem.at[slot]
        )

    def first_copy():
        return pltpu.make_async_copy(
            w_ref.at[pl.ds(0, first), :], wbuf.at[0, pl.ds(0, first), :], wsem.at[0]
        )

    inputs = [
        pltpu.make_async_copy(h_ref, hbuf, insem.at[0]),
        pltpu.make_async_copy(gain_ref, gbuf, insem.at[1]),
        pltpu.make_async_copy(draft_ref, draft_s, insem.at[2]),
        pltpu.make_async_copy(temp_ref, temp_s, insem.at[3]),
    ]
    for copy in inputs:
        copy.start()
    first_copy().start(priority=1)
    for i in range(1, SLOTS):
        tile_copy(i).start(priority=1)

    barrier = pltpu.get_barrier_semaphore()
    peers = []
    for j in range(1, 8):
        peer_dp = 1 - dp if j >= 4 else dp
        peer_tp = tp if j % 4 == 0 else (mate if j % 4 == 1 else None)
        if j % 4 == 2:
            peer_tp = lax.rem(tp + 2, 4)
        elif j % 4 == 3:
            peer_tp = lax.rem(mate + 2, 4)
        peers.append((peer_dp, peer_tp))
        pl.semaphore_signal(barrier, inc=1, device_id=(peer_dp, peer_tp), device_id_type=MESH)

    for copy in inputs:
        copy.wait()
    hidden = hbuf[...].astype(jnp.float32)
    hsend[...] = hidden

    lane = lax.broadcasted_iota(jnp.int32, (1, 128), 1)
    inner = lax.rem(lane, 64)
    temp_row = jnp.ones((1, 128), jnp.float32)
    draft_row = jnp.full((1, 128), -1, jnp.int32)
    for b in range(batch):
        temp_row = jnp.where(inner // positions == b, temp_s[0, b], temp_row)
        for p in range(positions - 1):
            draft_row = jnp.where(inner == b * positions + p, draft_s[b, p], draft_row)
    aux[0:1, :] = temp_row
    aux[1:2, :] = draft_row.astype(jnp.float32)
    aux[2:8, :] = jnp.zeros((6, 128), jnp.float32)

    def normed(block, at):
        mean_sq = jnp.mean(block * block, axis=-1, keepdims=True)
        inverse_rms = lax.rsqrt(mean_sq + NORM_EPS)
        gain = gbuf[...].astype(jnp.float32)
        for k in range(dim // 128):
            columns = slice(k * 128, (k + 1) * 128)
            scaled = block[:, columns] * inverse_rms * gain[k:k + 1, :]
            g[at:at + tokens, columns] = scaled.astype(jnp.bfloat16)

    g[...] = jnp.zeros_like(g)
    normed(hidden, 0)

    pl.semaphore_wait(barrier, 7)
    half = tokens // 2
    chunks = half // CHUNK

    def rows_of(which, k):
        return pl.ds(pl.multiple_of(which * half + k * CHUNK, CHUNK), CHUNK)

    def partner_copy(k):
        return pltpu.make_async_remote_copy(
            src_ref=hsend.at[rows_of(core, k), :], dst_ref=hrecv.at[rows_of(core, k), :],
            send_sem=send_sem.at[k], recv_sem=recv_sem.at[k],
            device_id=(1 - dp, tp), device_id_type=MESH,
        )

    def forward_copy(k):
        return pltpu.make_async_remote_copy(
            src_ref=hrecv.at[rows_of(core, k), :], dst_ref=hrecv.at[rows_of(core, k), :],
            send_sem=fsend_sem.at[k], recv_sem=frecv_sem.at[k],
            device_id=(dp, mate), device_id_type=MESH,
        )

    def forwarded_in(k):
        return pltpu.make_async_remote_copy(
            src_ref=hrecv.at[rows_of(1 - core, k), :], dst_ref=hrecv.at[rows_of(1 - core, k), :],
            send_sem=fsend_sem.at[k], recv_sem=frecv_sem.at[k],
            device_id=(dp, mate), device_id_type=MESH,
        )

    aux_copy = pltpu.make_async_remote_copy(
        src_ref=aux, dst_ref=auxin, send_sem=asem.at[0], recv_sem=asem.at[1],
        device_id=(1 - dp, tp), device_id_type=MESH,
    )
    aux_copy.start()
    for k in range(chunks):
        partner_copy(k).start()

    def scored(block, start, carry, scale, draft):
        top, total_exp, weighted, picked = carry
        groups = block.shape[0] // 8
        logits = lax.dot_general(
            block, g[...], (((1,), (1,)), ((), ())), preferred_element_type=jnp.float32
        ).reshape(groups, 8, 128)
        new_top = jnp.maximum(top, jnp.max(logits, axis=0))
        decay = jnp.exp2((top - new_top) * scale)
        shifted = jnp.exp2((logits - new_top[None]) * scale[None])
        total_exp = total_exp * decay + jnp.sum(shifted, axis=0)
        weighted = weighted * decay + jnp.sum(shifted * logits, axis=0)
        row = lax.broadcasted_iota(jnp.int32, (groups, 8, 128), 0) * 8 + lax.broadcasted_iota(
            jnp.int32, (groups, 8, 128), 1
        )
        picked = picked + jnp.sum(jnp.where(row == (draft - start)[None], logits, 0.0), axis=0)
        return new_top, total_exp, weighted, picked

    def body(i, carry, scale, draft):
        tile_copy(i).wait()
        start = tp * rows + offset(i) + jnp.where(i > PRIVATE_TILES, dp * shared, 0)
        carry = scored(wbuf[lax.rem(i, SLOTS)], start, carry, scale, draft)

        @pl.when(i + SLOTS < total)
        def _():
            tile_copy(i + SLOTS).start(priority=1)

        return carry

    zero = jnp.zeros((8, 128), jnp.float32)
    scale = jnp.broadcast_to(LOG2E / temp_row, (8, 128))
    draft = jnp.broadcast_to(draft_row, (8, 128))
    carry = (zero + LOWEST, zero, zero, zero)
    first_copy().wait()
    carry = scored(wbuf[0, 0:first, :], tp * rows, carry, scale, draft)
    tile_copy(SLOTS).start(priority=1)
    for i in range(1, PRIVATE_TILES + 1):
        carry = body(i, carry, scale, draft)
        if i >= 2 and i - 2 < chunks:
            partner_copy(i - 2).wait_recv()
            forward_copy(i - 2).start()

    aux_copy.wait()
    for k in range(chunks):
        if k > PRIVATE_TILES - 2:
            partner_copy(k).wait_recv()
            forward_copy(k).start()
    for k in range(chunks):
        forwarded_in(k).wait_recv()
    normed(hrecv[...], 64)

    own = lax.broadcasted_iota(jnp.int32, (8, 128), 1) < 64
    temp_row = jnp.where(lane < 64, temp_row, auxin[0:1, :])
    draft_row = jnp.where(lane < 64, draft_row, auxin[1:2, :].astype(jnp.int32))
    scale = jnp.broadcast_to(LOG2E / temp_row, (8, 128))
    draft = jnp.broadcast_to(draft_row, (8, 128))
    top, total_exp, weighted, picked = carry
    carry = (
        jnp.where(own, top, LOWEST), jnp.where(own, total_exp, 0.0),
        jnp.where(own, weighted, 0.0), jnp.where(own, picked, 0.0),
    )
    top, total_exp, weighted, picked = lax.fori_loop(
        1 + PRIVATE_TILES, total, functools.partial(body, scale=scale, draft=draft), carry
    )

    best = jnp.max(top, axis=0, keepdims=True)
    decay = jnp.exp2((top - best) * scale)
    stats[0:1, :] = best
    stats[1:2, :] = jnp.sum(total_exp * decay, axis=0, keepdims=True)
    stats[2:3, :] = jnp.sum(weighted * decay, axis=0, keepdims=True)
    stats[3:4, :] = jnp.sum(picked, axis=0, keepdims=True)
    stats[4:8, :] = jnp.zeros((4, 128), jnp.float32)

    def stats_copy(j):
        return pltpu.make_async_remote_copy(
            src_ref=stats, dst_ref=statsin.at[tp + 4 * (j // 4)],
            send_sem=ssend_sem.at[j], recv_sem=srecv_sem.at[j],
            device_id=peers[j - 1], device_id_type=MESH,
        )

    for j in range(1, 8):
        stats_copy(j).start()
    for k in range(chunks):
        partner_copy(k).wait_send()
        forward_copy(k).wait_send()
    statsin[tp] = stats[...]
    for j in range(1, 8):
        stats_copy(j).wait_recv()
    parts = [statsin[j] if j < 4 else pltpu.roll(statsin[j], 64, 1) for j in range(8)]
    best = functools.reduce(jnp.maximum, [part[0:1] for part in parts])
    scale, inverse = scale[0:1], 1.0 / temp_row
    decays = [jnp.exp2((part[0:1] - best) * scale) for part in parts]
    sum_exp = sum(part[1:2] * d for part, d in zip(parts, decays))
    sum_weighted = sum(part[2:3] * d for part, d in zip(parts, decays))
    pick = sum(part[3:4] for part in parts)
    log_norm = best * inverse + jnp.log(sum_exp)

    results = jnp.concatenate([
        pick * inverse - log_norm, log_norm, log_norm - sum_weighted / sum_exp * inverse,
        jnp.zeros((5, 128), jnp.float32),
    ])
    for b in range(batch):
        turned = results if b == 0 else pltpu.roll(results, 128 - b * positions, 1)
        lp_ref[b:b + 1, :] = turned[0:1, 0:positions - 1]
        lse_ref[b:b + 1, :] = turned[1:2, 0:positions]
        ent_ref[b:b + 1, :] = turned[2:3, 0:positions]
    for j in range(1, 8):
        stats_copy(j).wait_send()


def solution(mesh):
    def local_step(hidden, draft_ids, temperature, norm_gain, head_shard):
        batch, positions, dim = hidden.shape
        tokens = batch * positions
        any_spec = pl.BlockSpec(memory_space=pl.ANY)
        chunks = tokens // 2 // CHUNK
        return pl.pallas_call(
            kernel,
            out_shape=(
                jax.ShapeDtypeStruct((batch, positions - 1), jnp.float32),
                jax.ShapeDtypeStruct((batch, positions), jnp.float32),
                jax.ShapeDtypeStruct((batch, positions), jnp.float32),
            ),
            in_specs=[any_spec] * 5,
            out_specs=[pl.BlockSpec(memory_space=pltpu.VMEM)] * 3,
            scratch_shapes=[
                pltpu.VMEM((SLOTS, TILE, dim), jnp.bfloat16),
                pltpu.VMEM((tokens, dim), jnp.bfloat16),
                pltpu.VMEM((dim // 128, 128), jnp.bfloat16),
                pltpu.VMEM((tokens, dim), jnp.float32),
                pltpu.VMEM((tokens, dim), jnp.float32),
                pltpu.VMEM((128, dim), jnp.bfloat16),
                pltpu.VMEM((8, 128), jnp.float32),
                pltpu.VMEM((8, 128), jnp.float32),
                pltpu.VMEM((8, 128), jnp.float32),
                pltpu.VMEM((8, 8, 128), jnp.float32),
                pltpu.SMEM(draft_ids.shape, jnp.int32),
                pltpu.SMEM((1, batch), jnp.float32),
                pltpu.SemaphoreType.DMA((SLOTS,)),
                pltpu.SemaphoreType.DMA((4,)),
                pltpu.SemaphoreType.DMA((chunks,)),
                pltpu.SemaphoreType.DMA((chunks,)),
                pltpu.SemaphoreType.DMA((chunks,)),
                pltpu.SemaphoreType.DMA((chunks,)),
                pltpu.SemaphoreType.DMA((2,)),
                pltpu.SemaphoreType.DMA((8,)),
                pltpu.SemaphoreType.DMA((8,)),
            ],
            compiler_params=pltpu.CompilerParams(
                collective_id=0, has_side_effects=True, vmem_limit_bytes=65_000_000
            ),
            name="score",
        )(hidden.reshape(tokens, dim), draft_ids, temperature.reshape(1, batch), norm_gain.reshape(dim // 128, 128), head_shard)

    return jax.shard_map(
        local_step,
        mesh=mesh,
        in_specs=(P("dp", None, None), P("dp", None), P("dp"), P(None), P("tp", None)),
        out_specs=(P("dp", None), P("dp", None), P("dp", None)),
        check_vma=False,
    )
```
